32 devices in a mesh: rows: 8 (over z, y), sub: 4 (over x, core).
Axes of the slice: x: 2, y: 2, z: 4, core: 2. Of those that a mesh axis runs over, the one named last changes fastest.
Arguments:
- snapshots: float32 [513, 32768], P(None, ('rows', 'sub')), may hold values from -6 to 6
- start: float32 [512, 64], replicated, may hold values from -6 to 6
Outputs:
- modes: float32 [128, 32768], P(None, ('rows', 'sub'))
- operator: float32 [128, 128], replicated
- coefficients: float32 [128, 513], replicated
The draws below stay inside these ranges and needn't reach their ends.
All inputs are finite; a program needn't handle non-finite values.
Results may differ from the reference program's by a relative error of at most 0.0003.
Values sent between devices are 32-bit elements; how exact they have to be, the bound alone decides.
No kernel may reach another device: no remote copies, remote signals or barrier semaphores. Data moves between devices by JAX's collectives and lax.ppermute only.
A program may use at most 64 MiB of HBM per device.

```python
import jax
import jax.numpy as jnp
from jax import lax

SNAPS = 513
BLOCK = 64
STEPS = 2
RANK = 128
CELLS = 32768


def shard_levels(rng, shape, cuts, least, high):
    factor_of, own = 1.0, jax.random.fold_in(rng, 6)
    for position, blocks in cuts:
        steps = jnp.exp(jax.random.uniform(jax.random.fold_in(own, position), (blocks,), jnp.float32, least / len(cuts), high / len(cuts)))
        factor_of = factor_of * jnp.repeat(steps, shape[position] // blocks).reshape([-1 if axis == position else 1 for axis in range(len(shape))])
    return factor_of


def centred(rng, shape, scale, bound, cuts=(), kind=jnp.bfloat16):
    drawn = scale * jax.random.normal(rng, shape, jnp.float32)
    if cuts:
        drawn = drawn * shard_levels(rng, shape, cuts, -0.22, 0.18)
    return jnp.clip(drawn, -bound, bound).astype(kind)


def setup_inputs(seed: int = 0) -> dict:
    key_list = jax.random.split(jax.random.key(seed), 3)
    return {
        "snapshots": centred(key_list[0], (SNAPS, CELLS), 1.0, 6.0, ((1, 32),), jnp.float32),
        "start": centred(key_list[1], (SNAPS - 1, BLOCK), 1.0, 6.0, (), jnp.float32),
    }


def cross_cells(left, right):
    return lax.dot_general(left.astype(jnp.float32), right.astype(jnp.float32), (((1,), (1,)), ((), ())), precision=lax.Precision.HIGHEST, preferred_element_type=jnp.float32)

def matmul(left, right):
    return jnp.dot(left.astype(jnp.float32), right.astype(jnp.float32), precision=lax.Precision.HIGHEST, preferred_element_type=jnp.float32)

def factor_inverse(gram_block):
    factor = jnp.linalg.cholesky(gram_block)
    identity = jnp.eye(gram_block.shape[0], dtype=jnp.float32)
    inverse = jax.scipy.linalg.solve_triangular(factor, identity, lower=True)
    return (factor, inverse)

def orthonormal_columns(matrix):
    factor, inverse = factor_inverse(matmul(matrix.T, matrix))
    return matmul(matrix, inverse.T)

def reference(snapshots, start):
    width = start.shape[1]
    count = snapshots.shape[0]
    right_block = orthonormal_columns(start)
    right_blocks = [right_block]
    left_blocks = []
    columns = []
    for step in range(STEPS):
        padded = jnp.concatenate([right_block, jnp.zeros((1, width), jnp.float32)], 0)
        image = matmul(padded.T, snapshots)
        pieces = []
        if step > 0:
            earlier = jnp.concatenate(left_blocks, 0)
            coupling = cross_cells(earlier, image)
            image = image - matmul(coupling.T, earlier)
            pieces.append(coupling)
        factor, inverse = factor_inverse(cross_cells(image, image))
        left_blocks.append(matmul(inverse, image))
        pieces.append(factor.T)
        below = RANK - (step + 1) * width
        if below > 0:
            pieces.append(jnp.zeros((below, width), jnp.float32))
        columns.append(jnp.concatenate(pieces, 0))
        if step < STEPS - 1:
            back_sum = cross_cells(snapshots, left_blocks[-1])[:count - 1]
            basis = jnp.concatenate(right_blocks, 1)
            back_sum = back_sum - matmul(basis, matmul(basis.T, back_sum))
            right_block = orthonormal_columns(back_sum)
            right_blocks.append(right_block)
    triangle = jnp.concatenate(columns, 1)
    inverse_tri = jax.scipy.linalg.solve_triangular(triangle, jnp.eye(RANK, dtype=jnp.float32), lower=False)
    basis = jnp.concatenate(right_blocks, 1)
    shifted = jnp.concatenate([jnp.zeros((1, RANK), jnp.float32), basis], 0)
    advanced = matmul(shifted.T, snapshots)
    left_all = jnp.concatenate(left_blocks, 0)
    operator = matmul(cross_cells(left_all, advanced), inverse_tri)
    scale = jnp.sqrt(jnp.asarray(CELLS, jnp.float32))
    modes = scale * matmul(inverse_tri.T, advanced)
    mode_gram = cross_cells(modes, modes)
    mode_rhs = cross_cells(modes, snapshots)
    coefficients = jax.scipy.linalg.cho_solve((jnp.linalg.cholesky(mode_gram), True), mode_rhs)
    return (modes, operator, coefficients)
```

```python
import jax
import jax.numpy as jnp
from jax import lax
from jax.sharding import PartitionSpec as P

AXES = ("rows", "sub")
STEPS = 2
TILE = 128
SCATTERED = 3


def matmul(left, right):
    return jnp.dot(left, right, precision=lax.Precision.HIGHEST, preferred_element_type=jnp.float32)


def cross(left, right, dims):
    return lax.dot_general(
        left, right, (dims, ((), ())), precision=lax.Precision.HIGHEST, preferred_element_type=jnp.float32
    )


def exchange_mask(bit):
    return 3 << (bit - 1) if bit >= 4 and bit % 2 == 0 else 1 << bit


def sum_over_devices(part, devices):
    bits = devices.bit_length() - 1
    if 1 << bits != devices:
        return lax.psum(part, AXES)
    me = lax.axis_index(AXES)
    scattered = min(SCATTERED, bits)

    def swap(value, mask):
        return lax.ppermute(value, AXES, [(i, i ^ mask) for i in range(devices)])

    for bit in range(scattered):
        upper = (me >> bit) & 1
        half = part.shape[0] // 2
        kept = lax.dynamic_slice_in_dim(part, upper * half, half, 0)
        sent = lax.dynamic_slice_in_dim(part, (1 - upper) * half, half, 0)
        part = kept + swap(sent, exchange_mask(bit))
    for bit in range(scattered, bits):
        part = part + swap(part, exchange_mask(bit))
    for bit in reversed(range(scattered)):
        upper = (me >> bit) & 1
        other = swap(part, exchange_mask(bit))
        part = jnp.where(upper == 1, jnp.concatenate([other, part], 0), jnp.concatenate([part, other], 0))
    return part


def pack_symmetric(gram, last):
    tiles = gram.shape[0] // TILE
    pieces = [
        gram[i * TILE : (i + 1) * TILE, j * TILE : (j + 1) * TILE] for i in range(tiles) for j in range(i, tiles)
    ]
    tail = last.reshape(-1)
    unit = TILE * 8 << SCATTERED
    flat_rows = len(pieces) * TILE
    total = -(-(flat_rows * TILE + tail.size) // unit) * unit
    tail = jnp.pad(tail, (0, total - flat_rows * TILE - tail.size)).reshape(-1, TILE)
    return jnp.concatenate(pieces + [tail], 0)


def unpack_symmetric(packed, size):
    tiles = size // TILE
    grid = [[None] * tiles for _ in range(tiles)]
    at = 0
    for i in range(tiles):
        for j in range(i, tiles):
            tile = packed[at * TILE : (at + 1) * TILE]
            grid[i][j] = tile
            if j > i:
                grid[j][i] = tile.T
            at += 1
    gram = jnp.concatenate([jnp.concatenate(row, 1) for row in grid], 0)
    last = packed[at * TILE :].reshape(-1)[: size + 1]
    top = jnp.concatenate([gram, last[:size, None]], 1)
    return jnp.concatenate([top, last[None, :]], 0)


def lower_inverse(gram):
    factor = jnp.linalg.cholesky(gram)
    identity = jnp.eye(gram.shape[0], dtype=jnp.float32)
    return factor, jax.scipy.linalg.solve_triangular(factor, identity, lower=True)


def shards(snapshots, start):
    devices = lax.axis_size(AXES)
    size = snapshots.shape[0] - 1
    width = start.shape[1]
    total_cells = snapshots.shape[1] * devices
    past, future, final = snapshots[:size], snapshots[1:], snapshots[size:]

    local = cross(past, past, ((1,), (1,)))
    local_last = cross(final, snapshots, ((1,), (1,)))
    gram = unpack_symmetric(sum_over_devices(pack_symmetric(local, local_last), devices), size)

    _, start_inverse = lower_inverse(cross(start, start, ((0,), (0,))))
    right = cross(start, start_inverse, ((1,), (1,)))

    back = matmul(gram[:size, :size], right)
    inner = cross(right, back, ((0,), (0,)))
    back = (back - matmul(right, inner)) / jnp.diagonal(inner)[None, :]
    basis = jnp.concatenate([right, back], 1)
    order = STEPS * width
    early = matmul(gram[:, :size], basis)
    late = matmul(gram[:, 1:], basis)
    image_gram = cross(basis, early[:size], ((0,), (0,)))
    mixed = cross(basis, late[:size], ((0,), (0,)))
    advanced_gram = cross(basis, late[1:], ((0,), (0,)))
    image_factor, image_inverse = lower_inverse(image_gram)
    operator = matmul(matmul(image_inverse, mixed), image_inverse.T)
    scale = jnp.sqrt(jnp.asarray(total_cells, jnp.float32))
    weights = scale * cross(image_inverse, basis, ((1,), (1,)))
    modes = matmul(weights, future)
    advanced_factor = jnp.linalg.cholesky(advanced_gram)
    solved = jax.scipy.linalg.cho_solve((advanced_factor, True), late.T)
    coefficients = matmul(image_factor.T, solved) / scale
    return modes, operator, coefficients


def solution(mesh):
    return jax.shard_map(
        shards,
        mesh=mesh,
        in_specs=(P(None, AXES), P()),
        out_specs=(P(None, AXES), P(), P()),
        check_vma=False,
    )
```

```python
import jax
import jax.numpy as jnp
from jax import lax
from jax.experimental import pallas as pl
from jax.experimental.pallas import tpu as pltpu
from jax.sharding import PartitionSpec as P

AXES = ("rows", "sub")
STEPS = 2
TILE = 128
SCATTERED = 3


def exchange_mask(bit):
    return 3 << (bit - 1) if bit >= 4 and bit % 2 == 0 else 1 << bit


def sum_over_devices(part, devices):
    bits = devices.bit_length() - 1
    if 1 << bits != devices:
        return lax.psum(part, AXES)
    me = lax.axis_index(AXES)
    scattered = min(SCATTERED, bits)

    def swap(value, mask):
        return lax.ppermute(value, AXES, [(i, i ^ mask) for i in range(devices)])

    for bit in range(scattered):
        upper = (me >> bit) & 1
        half = part.shape[0] // 2
        kept = lax.dynamic_slice_in_dim(part, upper * half, half, 0)
        sent = lax.dynamic_slice_in_dim(part, (1 - upper) * half, half, 0)
        part = kept + swap(sent, exchange_mask(bit))
    for bit in range(scattered, bits):
        part = part + swap(part, exchange_mask(bit))
    for bit in reversed(range(scattered)):
        upper = (me >> bit) & 1
        other = swap(part, exchange_mask(bit))
        part = jnp.where(upper == 1, jnp.concatenate([other, part], 0), jnp.concatenate([part, other], 0))
    return part


def dot(left, right, dims=((1,), (0,))):
    return lax.dot_general(
        left, right, (dims, ((), ())), precision=lax.Precision.HIGHEST, preferred_element_type=jnp.float32
    )


NT = ((1,), (1,))


def packed_rows(size, devices):
    tiles = size // TILE
    used = tiles * (tiles + 1) // 2 * TILE + tiles + 1
    unit = 8 << SCATTERED
    return -(-used // unit) * unit


def gram_kernel(snapshots, packed):
    size = snapshots.shape[0] - 1
    tiles = size // TILE
    first = pl.program_id(0) == 0

    @pl.when(first)
    def _():
        packed[...] = jnp.zeros(packed.shape, jnp.float32)

    last = snapshots[size:, :]
    at = 0
    for i in range(tiles):
        wide = dot(snapshots[i * TILE : (i + 1) * TILE, :], snapshots[i * TILE : size, :], NT)
        for j in range(i, tiles):
            packed[at * TILE : (at + 1) * TILE, :] += wide[:, (j - i) * TILE : (j - i + 1) * TILE]
            at += 1
    edge = dot(jnp.broadcast_to(last, (8, last.shape[1])), snapshots[:size, :], NT)
    corner = jnp.sum(last * last, 1, keepdims=True)
    base = at * TILE
    for j in range(tiles):
        packed[base + j : base + j + 1, :] += edge[:1, j * TILE : (j + 1) * TILE]
    packed[base + tiles : base + tiles + 1, :] += jnp.broadcast_to(corner, (1, TILE))


def local_gram(snapshots, devices):
    count, cells = snapshots.shape
    rows = packed_rows(count - 1, devices)
    chunk = min(cells, 256)
    return pl.pallas_call(
        gram_kernel,
        grid=(cells // chunk,),
        in_specs=[pl.BlockSpec((count, chunk), lambda k: (0, k))],
        out_specs=pl.BlockSpec((rows, TILE), lambda k: (0, 0)),
        out_shape=jax.ShapeDtypeStruct((rows, TILE), jnp.float32),
        name="gram",
    )(snapshots)


def eliminate(squares, width):
    groups = width // 8
    lane = lax.broadcasted_iota(jnp.int32, (8, 2 * width), 1)
    sub = lax.broadcasted_iota(jnp.int32, (8, 2 * width), 0)
    work = []
    for square in squares:
        work.append(
            [
                jnp.where(lane < width, square[8 * g : 8 * g + 8], (lane == sub + (8 * g + width)).astype(jnp.float32))
                for g in range(groups)
            ]
        )

    def row(tile, i):
        return jnp.broadcast_to(tile[i : i + 1], (8, 2 * width))

    done = [[] for _ in squares]
    for p in range(groups):
        columns = [
            [
                {g: jnp.broadcast_to(rows[g][:, 8 * p + k : 8 * p + k + 1], (8, 2 * width)) for g in range(p, groups)}
                for k in range(8)
            ]
            for rows in work
        ]
        pivots = [jnp.ones((8, 2 * width), jnp.float32) for _ in work]
        for i in range(8):
            for m, rows in enumerate(work):
                cols = columns[m]
                pivot = row(cols[i][p], i)
                pivots[m] = jnp.where(sub == i, pivot, pivots[m])
                inverse = 1.0 / pivot
                factor = {g: cols[i][g] * inverse for g in range(p, groups)}
                factor[p] = jnp.where(sub > i, factor[p], 0.0)
                for k in range(i + 1, 8):
                    value = row(cols[k][p], i)
                    for g in range(p, groups):
                        cols[k][g] = cols[k][g] - factor[g] * value
                value = row(rows[p], i)
                for g in range(p, groups):
                    rows[g] = rows[g] - factor[g] * value
        for m, rows in enumerate(work):
            scaled = rows[p] * lax.rsqrt(pivots[m])
            done[m].append(jnp.where((lane < width) & (lane < sub + 8 * p), 0.0, scaled))
    return [jnp.concatenate(rows, 0) for rows in done]


def start_kernel(start, right):
    width = start.shape[1]
    value = start[...]
    gram = dot(value, value, ((0,), (0,)))
    (pair,) = eliminate([jnp.concatenate([gram, gram], 1)], width)
    right[...] = dot(pair[:, width:], value, NT)


def start_basis(start):
    size, width = start.shape
    return pl.pallas_call(
        start_kernel,
        out_shape=jax.ShapeDtypeStruct((width, size), jnp.float32),
        cost_estimate=pl.CostEstimate(flops=1 << 27, bytes_accessed=1 << 18, transcendentals=1 << 12),
        name="start_basis",
    )(start)


def finish_kernel(scale, packed, right, snapshots_hbm, modes, operator, coefficients, gram, snapshots, arrival):
    size = gram.shape[0]
    width = right.shape[0]
    order = 2 * width
    tiles = size // TILE
    fetch = pltpu.make_async_copy(snapshots_hbm, snapshots, arrival)
    fetch.start()

    at = 0
    for i in range(tiles):
        for j in range(i, tiles):
            tile = packed[at * TILE : (at + 1) * TILE, :]
            gram[i * TILE : (i + 1) * TILE, j * TILE : (j + 1) * TILE] = tile
            if j > i:
                gram[j * TILE : (j + 1) * TILE, i * TILE : (i + 1) * TILE] = tile.T
            at += 1
    base = at * TILE
    edge = jnp.concatenate([packed[base + j : base + j + 1, :] for j in range(tiles)], 1)
    corner = packed[base + tiles : base + tiles + 1, :]
    lane = lax.broadcasted_iota(jnp.int32, (width, size), 1)

    def shifted(block):
        ring = pltpu.roll(block, 1, 1)
        column = jnp.broadcast_to(ring[:, :1], (width, TILE))
        return jnp.where(lane == 0, 0.0, ring), column, ring

    def products(block):
        late, column, ring = shifted(block)
        both = dot(jnp.concatenate([block, late], 0), gram[...])
        early_product = both[:width]
        late_product = both[width:] + jnp.concatenate([column] * tiles, 1) * edge
        beyond = jnp.sum(late * edge, 1, keepdims=True) + column * corner
        late_ring = jnp.where(lane == 0, beyond[:, :1], late_product)
        return late, column, ring, early_product, late_product, beyond, late_ring

    first = right[...]
    late_a, column_a, ring_a, early_a, after_a, beyond_a, wrap_a = products(first)
    image_aa = dot(first, early_a, NT)
    diagonal = lax.broadcasted_iota(jnp.int32, (width, width), 0) == lax.broadcasted_iota(jnp.int32, (width, width), 1)
    norms = jnp.sum(jnp.where(diagonal, image_aa, 0.0), 1, keepdims=True)
    second = (early_a - dot(image_aa, first)) * (1.0 / norms)
    ahead_aa = dot(ring_a, wrap_a, NT)
    half_a = eliminate([jnp.concatenate([m, m], 1) for m in (image_aa, ahead_aa)], width)
    late_b, column_b, ring_b, early_b, after_b, beyond_b, wrap_b = products(second)

    basis = jnp.concatenate([first, second], 0)
    mixed = dot(basis, jnp.concatenate([after_a, after_b], 0), NT)
    image_b = dot(second, jnp.concatenate([early_a, early_b], 0), NT)
    ahead_b = dot(ring_b, jnp.concatenate([wrap_a, wrap_b], 0), NT)
    lower, schur = [], []
    for pair, side in ((half_a[0], image_b), (half_a[1], ahead_b)):
        link = dot(side[:, :width], pair[:, width:], NT)
        lower.append(link)
        schur.append(side[:, width:] - dot(link, link, NT))
    half_b = eliminate([jnp.concatenate([m, m], 1) for m in schur], width)

    def whole_inverse(pair_a, pair_b, link):
        corner_part = -dot(pair_b[:, width:], dot(link, pair_a[:, width:]))
        top = jnp.concatenate([pair_a[:, width:], jnp.zeros((width, width), jnp.float32)], 1)
        return jnp.concatenate([top, jnp.concatenate([corner_part, pair_b[:, width:]], 1)], 0)

    image_inverse = whole_inverse(half_a[0], half_b[0], lower[0])
    ahead_inverse = whole_inverse(half_a[1], half_b[1], lower[1])
    triangle = jnp.concatenate(
        [
            jnp.concatenate([half_a[0][:, :width], lower[0].T], 1),
            jnp.concatenate([jnp.zeros((width, width), jnp.float32), half_b[0][:, :width]], 1),
        ],
        0,
    )
    root = scale[0]
    shifted_basis = jnp.concatenate([late_a, late_b], 0)
    columns = jnp.concatenate([column_a, column_b], 0)
    weights = dot(image_inverse, jnp.concatenate([shifted_basis, columns], 1)) * root
    fetch.wait()
    final = snapshots[size:, :]
    cells = final.shape[1]
    tail = jnp.concatenate([weights[:, size:]] * (cells // TILE), 1) * final
    modes[...] = dot(weights[:, :size], snapshots[:size, :]) + tail

    operator[...] = dot(dot(image_inverse, mixed), image_inverse, NT)
    solver = dot(dot(triangle, ahead_inverse, NT), ahead_inverse) * (1.0 / root)
    ahead = jnp.concatenate(
        [jnp.concatenate([after_a, after_b], 0), jnp.concatenate([beyond_a, beyond_b], 0)], 1
    )
    coefficients[...] = dot(solver, ahead)[:, : size + 1]


def finish(packed, right, snapshots, total_cells):
    count, cells = snapshots.shape
    width, size = right.shape
    order = 2 * width
    scale = jnp.sqrt(jnp.full((1,), total_cells, jnp.float32))
    vmem = pl.BlockSpec(memory_space=pltpu.VMEM)
    return pl.pallas_call(
        finish_kernel,
        in_specs=[pl.BlockSpec(memory_space=pltpu.SMEM), vmem, vmem, pl.BlockSpec(memory_space=pl.ANY)],
        out_specs=[vmem, vmem, vmem],
        out_shape=[
            jax.ShapeDtypeStruct((order, cells), jnp.float32),
            jax.ShapeDtypeStruct((order, order), jnp.float32),
            jax.ShapeDtypeStruct((order, count), jnp.float32),
        ],
        scratch_shapes=[
            pltpu.VMEM((size, size), jnp.float32),
            pltpu.VMEM((count, cells), jnp.float32),
            pltpu.SemaphoreType.DMA(()),
        ],
        name="finish",
    )(scale, packed, right, snapshots)


def shards(snapshots, start):
    devices = lax.axis_size(AXES)
    total_cells = snapshots.shape[1] * devices
    right = start_basis(start)
    packed = sum_over_devices(local_gram(snapshots, devices), devices)
    return tuple(finish(packed, right, snapshots, total_cells))


def solution(mesh):
    return jax.shard_map(
        shards,
        mesh=mesh,
        in_specs=(P(None, AXES), P()),
        out_specs=(P(None, AXES), P(), P()),
        check_vma=False,
    )
```

```python
import jax
import jax.numpy as jnp
from jax import lax
from jax.experimental import pallas as pl
from jax.experimental.pallas import tpu as pltpu
from jax.sharding import PartitionSpec as P

AXES = ("rows", "sub")
STEPS = 2
TILE = 128
SCATTERED = 3


def exchange_mask(bit):
    return 3 << (bit - 1) if bit >= 4 and bit % 2 == 0 else 1 << bit


def swap(value, devices, mask):
    return lax.ppermute(value, AXES, [(i, i ^ mask) for i in range(devices)])


def sum_halves(kept, sent, devices, beside, operand):
    bits = devices.bit_length() - 1
    me = lax.axis_index(AXES)
    scattered = min(SCATTERED, bits)
    part = kept + swap(sent, devices, exchange_mask(0))
    for bit in range(1, scattered):
        upper = (me >> bit) & 1
        half = part.shape[0] // 2
        kept = lax.dynamic_slice_in_dim(part, upper * half, half, 0)
        sent = lax.dynamic_slice_in_dim(part, (1 - upper) * half, half, 0)
        if bit == 1:
            sent, operand = lax.optimization_barrier((sent, operand))
        received = swap(sent, devices, exchange_mask(bit))
        if bit == 1:
            received, result = lax.optimization_barrier((received, beside(operand)))
        part = kept + received
    for bit in range(scattered, bits):
        part = part + swap(part, devices, exchange_mask(bit))
    for bit in reversed(range(1, scattered)):
        upper = (me >> bit) & 1
        other = swap(part, devices, exchange_mask(bit))
        part = jnp.where(upper == 1, jnp.concatenate([other, part], 0), jnp.concatenate([part, other], 0))
    return part, swap(part, devices, exchange_mask(0)), result


def dot(left, right, dims=((1,), (0,))):
    return lax.dot_general(
        left, right, (dims, ((), ())), precision=lax.Precision.HIGHEST, preferred_element_type=jnp.float32
    )


NT = ((1,), (1,))


def packed_rows(size, devices):
    tiles = size // TILE
    used = tiles * (tiles + 1) // 2 * TILE + tiles + 1
    unit = 8 << SCATTERED
    return -(-used // unit) * unit


def split(value):
    high = value.astype(jnp.bfloat16)
    return high, (value - high.astype(jnp.float32)).astype(jnp.bfloat16)


def gram_kernel(upper, snapshots_hbm, kept, sent, snapshots, packed, arrivals):
    count, cells = snapshots.shape
    size = count - 1
    tiles = size // TILE
    chunks = arrivals.shape[0]
    chunk = cells // chunks
    copies = [
        pltpu.make_async_copy(
            snapshots_hbm.at[:, c * chunk : (c + 1) * chunk],
            snapshots.at[:, c * chunk : (c + 1) * chunk],
            arrivals.at[c],
        )
        for c in range(chunks)
    ]
    for copy in copies:
        copy.start()
    used = tiles * (tiles + 1) // 2 * TILE
    packed[used:, :] = jnp.zeros((packed.shape[0] - used, TILE), jnp.float32)
    for c, copy in enumerate(copies):
        copy.wait()
        high, low = split(snapshots[:size, c * chunk : (c + 1) * chunk])
        right = jnp.concatenate([high, low, high], 1)
        left = jnp.concatenate([high, high, low], 1)
        last = snapshots[size:, c * chunk : (c + 1) * chunk]
        last_high, last_low = split(jnp.broadcast_to(last, (16, chunk)))
        edge = mxu(jnp.concatenate([last_high, last_high, last_low], 1), right)
        corner = jnp.sum(last * last, 1, keepdims=True)
        at = 0
        for i in range(tiles):
            wide = mxu(left[i * TILE : (i + 1) * TILE], right[i * TILE :])
            for j in range(i, tiles):
                piece = wide[:, (j - i) * TILE : (j - i + 1) * TILE]
                if c:
                    packed[at * TILE : (at + 1) * TILE, :] += piece
                else:
                    packed[at * TILE : (at + 1) * TILE, :] = piece
                at += 1
        for j in range(tiles):
            packed[used + j : used + j + 1, :] += edge[:1, j * TILE : (j + 1) * TILE]
        packed[used + tiles : used + tiles + 1, :] += jnp.broadcast_to(corner, (1, TILE))
    half = kept.shape[0]
    mine = pl.multiple_of(upper[0] * half, 8)
    kept[...] = packed[pl.ds(mine, half), :]
    sent[...] = packed[pl.ds(pl.multiple_of(half - mine, 8), half), :]


def mxu(left, right):
    return lax.dot_general(left, right, (NT, ((), ())), preferred_element_type=jnp.float32)


def local_gram(snapshots, devices):
    count, cells = snapshots.shape
    rows = packed_rows(count - 1, devices)
    chunks = max(1, cells // 256)
    upper = (lax.axis_index(AXES) & 1).astype(jnp.int32).reshape(1)
    return pl.pallas_call(
        gram_kernel,
        in_specs=[pl.BlockSpec(memory_space=pltpu.SMEM), pl.BlockSpec(memory_space=pl.ANY)],
        out_specs=[pl.BlockSpec(memory_space=pltpu.VMEM)] * 2,
        out_shape=[pltpu.VMEM((rows // 2, TILE), jnp.float32)] * 2,
        scratch_shapes=[
            pltpu.VMEM((count, cells), jnp.float32),
            pltpu.VMEM((rows, TILE), jnp.float32),
            pltpu.SemaphoreType.DMA((chunks,)),
        ],
        name="gram",
    )(upper, snapshots)


def eliminate(squares, width):
    groups = width // 8
    lane = lax.broadcasted_iota(jnp.int32, (8, 2 * width), 1)
    sub = lax.broadcasted_iota(jnp.int32, (8, 2 * width), 0)
    work = []
    for square in squares:
        work.append(
            [
                jnp.where(lane < width, square[8 * g : 8 * g + 8], (lane == sub + (8 * g + width)).astype(jnp.float32))
                for g in range(groups)
            ]
        )

    def row(tile, i):
        return jnp.broadcast_to(tile[i : i + 1], (8, 2 * width))

    done = [[] for _ in squares]
    for p in range(groups):
        columns = [
            [
                {g: jnp.broadcast_to(rows[g][:, 8 * p + k : 8 * p + k + 1], (8, 2 * width)) for g in range(p, groups)}
                for k in range(8)
            ]
            for rows in work
        ]
        pivots = [jnp.ones((8, 2 * width), jnp.float32) for _ in work]
        for i in range(8):
            for m, rows in enumerate(work):
                cols = columns[m]
                pivot = row(cols[i][p], i)
                pivots[m] = jnp.where(sub == i, pivot, pivots[m])
                inverse = 1.0 / pivot
                factor = {g: cols[i][g] * inverse for g in range(p, groups)}
                factor[p] = jnp.where(sub > i, factor[p], 0.0)
                for k in range(i + 1, 8):
                    value = row(cols[k][p], i)
                    for g in range(p, groups):
                        cols[k][g] = cols[k][g] - factor[g] * value
                value = row(rows[p], i)
                for g in range(p, groups):
                    rows[g] = rows[g] - factor[g] * value
        for m, rows in enumerate(work):
            scaled = rows[p] * lax.rsqrt(pivots[m])
            done[m].append(jnp.where((lane < width) & (lane < sub + 8 * p), 0.0, scaled))
    return [jnp.concatenate(rows, 0) for rows in done]


def start_kernel(start, right):
    width = start.shape[0]
    value = start[...]
    gram = dot(value, value, NT)
    (pair,) = eliminate([jnp.concatenate([gram, gram], 1)], width)
    right[...] = dot(pair[:, width:], value)


def start_basis(start):
    return pl.pallas_call(
        start_kernel,
        in_specs=[pl.BlockSpec(memory_space=pltpu.VMEM)],
        out_specs=pl.BlockSpec(memory_space=pltpu.VMEM),
        out_shape=pltpu.VMEM(start.shape, jnp.float32),
        name="start_basis",
    )(start)


def finish_kernel(
    upper, scale, mine, other, right, snapshots_hbm, modes, operator, coefficients, packed, gram, snapshots, arrival
):
    size = gram.shape[0]
    width = right.shape[0]
    order = 2 * width
    tiles = size // TILE
    fetch = pltpu.make_async_copy(snapshots_hbm, snapshots, arrival)
    fetch.start()

    half = mine.shape[0]
    place = pl.multiple_of(upper[0] * half, 8)
    packed[pl.ds(place, half), :] = mine[...]
    packed[pl.ds(pl.multiple_of(half - place, 8), half), :] = other[...]
    at = 0
    for i in range(tiles):
        for j in range(i, tiles):
            tile = packed[at * TILE : (at + 1) * TILE, :]
            gram[i * TILE : (i + 1) * TILE, j * TILE : (j + 1) * TILE] = tile
            if j > i:
                gram[j * TILE : (j + 1) * TILE, i * TILE : (i + 1) * TILE] = tile.T
            at += 1
    base = at * TILE
    edge = jnp.concatenate([packed[base + j : base + j + 1, :] for j in range(tiles)], 1)
    corner = packed[base + tiles : base + tiles + 1, :]
    lane = lax.broadcasted_iota(jnp.int32, (width, size), 1)

    def shifted(block):
        ring = pltpu.roll(block, 1, 1)
        column = jnp.broadcast_to(ring[:, :1], (width, TILE))
        return jnp.where(lane == 0, 0.0, ring), column, ring

    def products(block):
        late, column, ring = shifted(block)
        both = dot(jnp.concatenate([block, late], 0), gram[...])
        early_product = both[:width]
        late_product = both[width:] + jnp.concatenate([column] * tiles, 1) * edge
        beyond = jnp.sum(late * edge, 1, keepdims=True) + column * corner
        late_ring = jnp.where(lane == 0, beyond[:, :1], late_product)
        return late, column, ring, early_product, late_product, beyond, late_ring

    first = right[...]
    late_a, column_a, ring_a, early_a, after_a, beyond_a, wrap_a = products(first)
    image_aa = dot(first, early_a, NT)
    diagonal = lax.broadcasted_iota(jnp.int32, (width, width), 0) == lax.broadcasted_iota(jnp.int32, (width, width), 1)
    norms = jnp.sum(jnp.where(diagonal, image_aa, 0.0), 1, keepdims=True)
    second = (early_a - dot(image_aa, first)) * (1.0 / norms)
    ahead_aa = dot(ring_a, wrap_a, NT)
    half_a = eliminate([jnp.concatenate([m, m], 1) for m in (image_aa, ahead_aa)], width)
    late_b, column_b, ring_b, early_b, after_b, beyond_b, wrap_b = products(second)

    basis = jnp.concatenate([first, second], 0)
    mixed = dot(basis, jnp.concatenate([after_a, after_b], 0), NT)
    image_b = dot(second, jnp.concatenate([early_a, early_b], 0), NT)
    ahead_b = dot(ring_b, jnp.concatenate([wrap_a, wrap_b], 0), NT)
    lower, schur = [], []
    for pair, side in ((half_a[0], image_b), (half_a[1], ahead_b)):
        link = dot(side[:, :width], pair[:, width:], NT)
        lower.append(link)
        schur.append(side[:, width:] - dot(link, link, NT))
    half_b = eliminate([jnp.concatenate([m, m], 1) for m in schur], width)

    def whole_inverse(pair_a, pair_b, link):
        corner_part = -dot(pair_b[:, width:], dot(link, pair_a[:, width:]))
        top = jnp.concatenate([pair_a[:, width:], jnp.zeros((width, width), jnp.float32)], 1)
        return jnp.concatenate([top, jnp.concatenate([corner_part, pair_b[:, width:]], 1)], 0)

    image_inverse = whole_inverse(half_a[0], half_b[0], lower[0])
    ahead_inverse = whole_inverse(half_a[1], half_b[1], lower[1])
    triangle = jnp.concatenate(
        [
            jnp.concatenate([half_a[0][:, :width], lower[0].T], 1),
            jnp.concatenate([jnp.zeros((width, width), jnp.float32), half_b[0][:, :width]], 1),
        ],
        0,
    )
    root = scale[0]
    shifted_basis = jnp.concatenate([late_a, late_b], 0)
    columns = jnp.concatenate([column_a, column_b], 0)
    weights = dot(image_inverse, jnp.concatenate([shifted_basis, columns], 1)) * root
    fetch.wait()
    final = snapshots[size:, :]
    cells = final.shape[1]
    tail = jnp.concatenate([weights[:, size:]] * (cells // TILE), 1) * final
    modes[...] = dot(weights[:, :size], snapshots[:size, :]) + tail

    operator[...] = dot(dot(image_inverse, mixed), image_inverse, NT)
    solver = dot(dot(triangle, ahead_inverse, NT), ahead_inverse) * (1.0 / root)
    ahead = jnp.concatenate(
        [jnp.concatenate([after_a, after_b], 0), jnp.concatenate([beyond_a, beyond_b], 0)], 1
    )
    coefficients[...] = dot(solver, ahead).T[: size + 1]


def finish(mine, other, right, snapshots, total_cells):
    count, cells = snapshots.shape
    width, size = right.shape
    order = 2 * width
    scale = jnp.sqrt(jnp.full((1,), total_cells, jnp.float32))
    upper = (lax.axis_index(AXES) & 1).astype(jnp.int32).reshape(1)
    smem = pl.BlockSpec(memory_space=pltpu.SMEM)
    vmem = pl.BlockSpec(memory_space=pltpu.VMEM)
    mine, other, right = (pltpu.with_memory_space_constraint(v, pltpu.VMEM) for v in (mine, other, right))
    return pl.pallas_call(
        finish_kernel,
        in_specs=[smem, smem, vmem, vmem, vmem, pl.BlockSpec(memory_space=pl.ANY)],
        out_specs=[vmem, vmem, vmem],
        out_shape=[
            jax.ShapeDtypeStruct((order, cells), jnp.float32),
            jax.ShapeDtypeStruct((order, order), jnp.float32),
            jax.ShapeDtypeStruct((count, order), jnp.float32),
        ],
        scratch_shapes=[
            pltpu.VMEM((2 * mine.shape[0], TILE), jnp.float32),
            pltpu.VMEM((size, size), jnp.float32),
            pltpu.VMEM((count, cells), jnp.float32),
            pltpu.SemaphoreType.DMA(()),
        ],
        name="finish",
    )(upper, scale, mine, other, right, snapshots)


def shards(snapshots, start):
    devices = lax.axis_size(AXES)
    total_cells = snapshots.shape[1] * devices
    kept, sent = local_gram(snapshots, devices)
    mine, other, right = sum_halves(kept, sent, devices, start_basis, start.T)
    modes, operator, coefficients = finish(mine, other, right, snapshots, total_cells)
    return modes, operator, coefficients.T


def solution(mesh):
    return jax.shard_map(
        shards,
        mesh=mesh,
        in_specs=(P(None, AXES), P()),
        out_specs=(P(None, AXES), P(), P()),
        check_vma=False,
    )
```
